512 devices in a mesh: unit: 2 (over core), zero: 16 (over z), model: 16 (over y, x).
Axes of the slice: x: 4, y: 4, z: 16, core: 2. Of those that a mesh axis runs over, the one named last changes fastest.
Arguments:
- first_query: float32 [16384, 8192], P(('unit', 'zero'), 'model'), parts along dimension 0, may hold values from -0.09375 to 0.09375
- second_query: float32 [16384, 8192], P(('unit', 'zero'), 'model'), parts along dimension 0, may hold values from -0.0625 to 0.0625
- first_key: float32 [16384, 1024], P(('unit', 'zero'), 'model'), parts along dimension 0, may hold values from -0.09375 to 0.09375
- second_key: float32 [16384, 1024], P(('unit', 'zero'), 'model'), parts along dimension 0, may hold values from -0.0625 to 0.0625
- first_value: float32 [16384, 1024], P(('unit', 'zero'), 'model'), parts along dimension 0, may hold values from -0.09375 to 0.09375
- second_value: float32 [16384, 1024], P(('unit', 'zero'), 'model'), parts along dimension 0, may hold values from -0.0625 to 0.0625
- mix_share: float32 [16384], P(('unit', 'zero')), parts along dimension 0, may hold values from 0.2 to 0.8
- norm_train: float32 [16384], P(('unit', 'zero', 'model')), parts along dimension 0, may hold values from 0.25 to 1.75
- norm_step: float32 [16384], P(('unit', 'zero', 'model')), parts along dimension 0, may hold values from -0.3 to 0.3
Outputs:
- serve_query: bfloat16 [16384, 8192], P('unit', 'model'), parts along dimension 0
- serve_key: bfloat16 [16384, 1024], P('unit', 'model'), parts along dimension 0
- serve_value: bfloat16 [16384, 1024], P('unit', 'model'), parts along dimension 0
- factor_query: float32 [16384], P(('unit', 'model')), parts along dimension 0
- factor_key: float32 [2048], P(('unit', 'model')), parts along dimension 0
- factor_value: float32 [2048], P(('unit', 'model')), parts along dimension 0
- serve_norm: bfloat16 [16384], P('unit'), parts along dimension 0
The draws below stay inside these ranges and needn't reach their ends.
There are 2 independent parts, one for each index of `unit`. The reference program is written for one: setup_inputs(seed, part) draws one part's arguments, and reference() takes and returns one part's arrays. A program takes and returns all parts, laid end to end along the dimension named above; each array names one. Nothing has to cross between parts.
All inputs are finite; a program needn't handle non-finite values.
Results may differ from the reference program's by a relative error of at most 0.0004.
Values may be sent and summed in bfloat16 or wider, within the bound.
A program may use at most 128 MiB of HBM per device.

```python
import jax
import jax.numpy as jnp
from jax import lax

D_MODEL = 8192
Q_DIM = 8192
KV_DIM = 1024


def with_spikes(values, rng, source, target, shards_of, factor):
    owner, partner = [(jnp.arange(values.shape[dim]) // (values.shape[dim] // shards_of)).reshape([-1 if axis == dim else 1 for axis in range(values.ndim)]) for dim in (source, target)]
    chosen = jax.random.permutation(rng, shards_of)[partner]
    strong = (owner == chosen) | (owner == (partner + shards_of // 2) % shards_of)
    return jnp.where(strong, factor * values, values)


def level_of(rng, shape, cuts, smallest, high):
    def one(axis_at, blocks):
        draws = jax.random.uniform(jax.random.fold_in(jax.random.fold_in(rng, 6), axis_at), (blocks,), jnp.float32, smallest / len(cuts), high / len(cuts))
        return jnp.repeat(jnp.exp(draws), shape[axis_at] // blocks).reshape((-1,) + (1,) * (len(shape) - axis_at - 1))

    loudness = one(*cuts[0])
    for cut in cuts[1:]:
        loudness = loudness * one(*cut)
    return loudness


def normal_values(stream_key, extent, deviation, reach, cuts=(), dtype=jnp.bfloat16):
    entries = deviation * jax.random.normal(stream_key, extent, jnp.float32)
    if cuts:
        entries = entries * level_of(stream_key, extent, cuts, -0.22, 0.18)
    return jnp.clip(entries, -reach, reach).astype(dtype)


def noise_with(own_key, extent, deviation, most, cuts, heavy, held_as=jnp.bfloat16):
    values = deviation * jax.random.normal(own_key, extent, jnp.float32)
    if cuts:
        values = values * level_of(own_key, extent, cuts, -0.22, 0.18)
    return jnp.clip(with_spikes(values, jax.random.fold_in(own_key, 3), *heavy), -most, most).astype(held_as)


def setup_inputs(seed: int = 0, part: int = 0) -> dict:
    key_list = jax.random.split(jax.random.key(seed), 10)
    own_keys = jax.random.split(jax.random.fold_in(key_list[9], part), 10)
    return {
        "first_query": noise_with(own_keys[0], (D_MODEL, Q_DIM), D_MODEL ** -0.5, 0.09375, ((0, 16), (1, 16)), (0, 1, 16, 2.0), jnp.float32),
        "second_query": normal_values(own_keys[1], (D_MODEL, Q_DIM), D_MODEL ** -0.5, 0.0625, ((0, 16), (1, 16)), jnp.float32),
        "first_key": noise_with(own_keys[2], (D_MODEL, KV_DIM), D_MODEL ** -0.5, 0.09375, ((0, 16), (1, 16)), (0, 1, 16, 2.0), jnp.float32),
        "second_key": normal_values(own_keys[3], (D_MODEL, KV_DIM), D_MODEL ** -0.5, 0.0625, ((0, 16), (1, 16)), jnp.float32),
        "first_value": noise_with(own_keys[4], (D_MODEL, KV_DIM), D_MODEL ** -0.5, 0.09375, ((0, 16), (1, 16)), (0, 1, 16, 2.0), jnp.float32),
        "second_value": normal_values(own_keys[5], (D_MODEL, KV_DIM), D_MODEL ** -0.5, 0.0625, ((0, 16), (1, 16)), jnp.float32),
        "mix_share": jnp.clip(0.2 + 0.6 * jax.random.uniform(own_keys[6], (D_MODEL,), jnp.float32) ** level_of(own_keys[6], (D_MODEL,), ((0, 16),), -0.2, 0.2), 0.2, 0.8),
        "norm_train": jnp.clip(1.0 + 0.15 * jax.random.normal(own_keys[7], (D_MODEL,), jnp.float32), 0.25, 1.75),
        "norm_step": jnp.clip(jax.random.uniform(own_keys[8], (D_MODEL,), jnp.float32, -0.3, 0.3) * level_of(own_keys[8], (D_MODEL,), ((0, 256),), -0.4, 0.0), -0.3, 0.3),
    }


def reference(first_query, second_query, first_key, second_key, first_value, second_value, mix_share, norm_train, norm_step):
    fresh_query = mix_share[:, None] * first_query + (1.0 - mix_share[:, None]) * second_query
    fresh_key = mix_share[:, None] * first_key + (1.0 - mix_share[:, None]) * second_key
    fresh_value = mix_share[:, None] * first_value + (1.0 - mix_share[:, None]) * second_value
    factor_query = jnp.sqrt(lax.optimization_barrier(jnp.sum(fresh_query * fresh_query, axis=0)))
    serve_query = (fresh_query / factor_query).astype(jnp.bfloat16)
    factor_key = jnp.sqrt(lax.optimization_barrier(jnp.sum(fresh_key * fresh_key, axis=0)))
    serve_key = (fresh_key / factor_key).astype(jnp.bfloat16)
    factor_value = jnp.sqrt(lax.optimization_barrier(jnp.sum(fresh_value * fresh_value, axis=0)))
    serve_value = (fresh_value / factor_value).astype(jnp.bfloat16)
    serve_norm = (norm_train + norm_step).astype(jnp.bfloat16)
    return (serve_query, serve_key, serve_value, factor_query, factor_key, factor_value, serve_norm)
```

```python
import functools

import jax
import jax.numpy as jnp
from jax import lax
from jax.experimental import pallas as pl
from jax.experimental.pallas import tpu as pltpu
from jax.sharding import PartitionSpec as P

MESH = pl.DeviceIdType.MESH
LANES = 128
PIECES = 10


def gather_kernel(
    first_q, second_q, first_k, second_k, first_v, second_v, mix, train, step,
    blocks, factors, norm,
    a_q, b_q, a_kv, b_kv, mix_row, share, norm_in, lane_row, fresh, stat, plane, norm_wide,
    load_sem, stat_send, stat_recv, plane_send, plane_recv,
    right_send, right_recv, left_send, left_recv,
):
    n, m = lax.axis_size("zero"), lax.axis_size("model")
    me, col = lax.axis_index("zero"), lax.axis_index("model")
    rows, cols = first_q.shape
    thin = first_k.shape[0]
    wide = rows + 2 * thin
    size = wide // PIECES
    half = PIECES // 2
    tiles = rows // LANES

    barrier = pltpu.get_barrier_semaphore()

    def greet_line(d, c):
        pl.semaphore_signal(barrier, inc=1, device_id={"zero": lax.rem(me + d, n)}, device_id_type=MESH)
        return c

    def greet_plane(d, c):
        pl.semaphore_signal(barrier, inc=1, device_id={"model": lax.rem(col + d, m)}, device_id_type=MESH)
        return c

    lax.fori_loop(1, n, greet_line, 0)
    lax.fori_loop(1, m, greet_plane, 0)

    loads = [pltpu.make_async_copy(mix, mix_row, load_sem.at[0])]
    for r in range(tiles):
        part = pl.ds(r * LANES, LANES)
        loads.append(pltpu.make_async_copy(first_q.at[part], a_q.at[part], load_sem.at[1 + 2 * r]))
        loads.append(pltpu.make_async_copy(second_q.at[part], b_q.at[part], load_sem.at[2 + 2 * r]))
    at = 1 + 2 * tiles
    for k, (src, dst) in enumerate(
        (
            (first_k, a_kv.at[pl.ds(0, thin)]),
            (first_v, a_kv.at[pl.ds(thin, thin)]),
            (second_k, b_kv.at[pl.ds(0, thin)]),
            (second_v, b_kv.at[pl.ds(thin, thin)]),
            (train, norm_in.at[0]),
            (step, norm_in.at[1]),
        )
    ):
        loads.append(pltpu.make_async_copy(src, dst, load_sem.at[at + k]))
    for load in loads:
        load.start()

    loads[0].wait()
    for r in range(tiles):
        row = mix_row[:, r * LANES : (r + 1) * LANES]
        share[r * LANES : (r + 1) * LANES, :] = jnp.broadcast_to(row, (LANES, LANES)).T

    sums = [jnp.zeros((8, LANES), jnp.float32) for _ in range(tiles)]
    for r in range(tiles):
        loads[1 + 2 * r].wait()
        loads[2 + 2 * r].wait()
        part = slice(r * LANES, (r + 1) * LANES)
        w = share[part, :]
        for c in range(tiles):
            lanes = slice(c * LANES, (c + 1) * LANES)
            f = w * a_q[part, lanes] + (1.0 - w) * b_q[part, lanes]
            fresh[part, lanes] = f
            sums[c] = sums[c] + jnp.sum((f * f).reshape(LANES // 8, 8, LANES), axis=0)
    for load in loads[at : at + 4]:
        load.wait()
    w = mix_row[...]
    f = w * a_kv[...] + (1.0 - w) * b_kv[...]
    fresh[rows:, :] = f
    s = f * f
    folded = s[:, :LANES]
    for c in range(1, tiles):
        folded = folded + s[:, c * LANES : (c + 1) * LANES]
    thin_sum = jnp.sum(folded.T, axis=0, keepdims=True)

    for load in loads[at + 4 :]:
        load.wait()
    gain = (norm_in[0] + norm_in[1]).astype(jnp.bfloat16).astype(jnp.float32)
    lane_row[...] = jnp.zeros_like(lane_row)
    share_of_row = gain.shape[1]
    per_row = LANES // share_of_row
    lane_row[0:1, 0:share_of_row] = gain
    gain = lane_row[...]
    spread = gain
    for k in range(1, per_row):
        spread = spread + pltpu.roll(gain, k * share_of_row, 1)
    lane = lax.broadcasted_iota(jnp.int32, (8, LANES), 1)
    spread = jnp.where(lane // share_of_row == lax.rem(col, per_row), spread, 0.0)

    row_at = lax.broadcasted_iota(jnp.int32, (8, LANES), 0)
    mine = jnp.zeros((8, LANES), jnp.float32)
    for c in range(tiles):
        mine = jnp.where(row_at == c, jnp.sum(sums[c], axis=0, keepdims=True), mine)
    mine = jnp.where(row_at == tiles, thin_sum, mine)
    mine = jnp.where(row_at == tiles + 1, spread[0:1, :], mine)
    stat[me] = mine

    pl.semaphore_wait(barrier, n - 1 + m - 1)

    def stat_copy(d):
        return pltpu.make_async_remote_copy(
            stat.at[me], stat.at[me], stat_send.at[d], stat_recv.at[me],
            device_id={"zero": lax.rem(me + d, n)}, device_id_type=MESH,
        )

    def stat_from(d):
        source = lax.rem(me + d, n)
        return pltpu.make_async_remote_copy(
            stat.at[source], stat.at[source], stat_send.at[d], stat_recv.at[source],
            device_id={"zero": source}, device_id_type=MESH,
        )

    def send_stat(d, c):
        stat_copy(d).start()
        return c

    def take_stat(d, c):
        stat_from(d).wait_recv()
        return c

    lax.fori_loop(1, n, send_stat, 0)
    lax.fori_loop(1, n, take_stat, 0)

    total = stat[0]
    for z in range(1, n):
        total = total + stat[z]
    factor = jnp.sqrt(total)
    factors[...] = factor
    inverse = 1.0 / factor
    thin_inverse = jnp.broadcast_to(inverse[tiles : tiles + 1, :], (LANES, LANES)).T

    def piece_copy(send, recv, origin, s, p, to):
        where = blocks.at[origin, pl.ds(p * size, size)]
        return pltpu.make_async_remote_copy(
            where, where, send.at[s * PIECES + p], recv.at[s * PIECES + p],
            device_id={"zero": to}, device_id_type=MESH,
        )

    after, before = lax.rem(me + 1, n), lax.rem(me + n - 1, n)

    def to_right(s, p):
        return piece_copy(right_send, right_recv, lax.rem(me + n - s, n), s, p, after)

    def to_left(s, p):
        return piece_copy(left_send, left_recv, lax.rem(me + s, n), s, p, before)

    def from_left(s, p):
        return piece_copy(right_send, right_recv, lax.rem(before + n - s, n), s, p, after)

    def from_right(s, p):
        return piece_copy(left_send, left_recv, lax.rem(after + s, n), s, p, before)

    for p in range(PIECES):
        low, high = p * size, (p + 1) * size
        edge = min(max(rows, low), high)
        if low < edge:
            for c in range(tiles):
                lanes = slice(c * LANES, (c + 1) * LANES)
                blocks[me, low:edge, lanes] = (fresh[low:edge, lanes] * inverse[c : c + 1, :]).astype(jnp.bfloat16)
        if edge < high:
            scale = thin_inverse[edge - rows : high - rows, :]
            for c in range(tiles):
                lanes = slice(c * LANES, (c + 1) * LANES)
                blocks[me, edge:high, lanes] = (fresh[edge:high, lanes] * scale).astype(jnp.bfloat16)
        to_right(0, p).start()
        to_left(0, p).start()

    plane[col] = stat[:, tiles + 1, :]

    def plane_copy(d):
        return pltpu.make_async_remote_copy(
            plane.at[col], plane.at[col], plane_send.at[d], plane_recv.at[col],
            device_id={"model": lax.rem(col + d, m)}, device_id_type=MESH,
        )

    def plane_from(d):
        source = lax.rem(col + d, m)
        return pltpu.make_async_remote_copy(
            plane.at[source], plane.at[source], plane_send.at[d], plane_recv.at[source],
            device_id={"model": source}, device_id_type=MESH,
        )

    def send_plane(d, c):
        plane_copy(d).start()
        return c

    def take_plane(d, c):
        plane_from(d).wait_recv()
        return c

    lax.fori_loop(1, m, send_plane, 0)

    last = n // 2 - 1

    def hop(s, c):
        def one(p, c):
            from_left(s - 1, p).wait_recv()
            to_right(s, p).start()
            from_right(s - 1, p).wait_recv()
            to_left(s, p).start()
            return c

        return lax.fori_loop(0, PIECES, one, c)

    lax.fori_loop(1, last, hop, 0)

    lax.fori_loop(1, m, take_plane, 0)
    per = m // per_row
    for k in range(per):
        line = plane[k * per_row]
        for j in range(1, per_row):
            line = line + plane[k * per_row + j]
        norm_wide[pl.ds(k, n, stride=per), :] = line
    norm[...] = norm_wide[...].astype(jnp.bfloat16)

    def near(p, c):
        from_left(last - 1, p).wait_recv()
        to_right(last, p).start()
        from_right(last - 1, p + half).wait_recv()
        to_left(last, p + half).start()
        return c

    def far(p, c):
        from_right(last - 1, p).wait_recv()
        from_left(last - 1, p + half).wait_recv()
        return c

    def end(p, c):
        from_left(last, p).wait_recv()
        from_right(last, p + half).wait_recv()
        return c

    lax.fori_loop(0, half, near, 0)
    lax.fori_loop(0, half, far, 0)
    lax.fori_loop(0, half, end, 0)

    def sent(s, c):
        def one(p, c):
            to_right(s, p).wait_send()
            to_left(s, p).wait_send()
            return c

        return lax.fori_loop(0, PIECES, one, c)

    def sent_last(p, c):
        to_right(last, p).wait_send()
        to_left(last, p + half).wait_send()
        return c

    def sent_small(d, c):
        stat_copy(d).wait_send()
        return c

    def sent_plane(d, c):
        plane_copy(d).wait_send()
        return c

    lax.fori_loop(0, last, sent, 0)
    lax.fori_loop(0, half, sent_last, 0)
    lax.fori_loop(1, n, sent_small, 0)
    lax.fori_loop(1, m, sent_plane, 0)


def place_kernel(n, rows, thin, blocks, factors, norm, query, key, value, f_query, f_key, f_value, norm_out, sems):
    copies = []
    for z in range(n):
        here = pl.ds(z * rows, rows)
        copies.append(pltpu.make_async_copy(blocks.at[z, pl.ds(0, rows)], query.at[here], sems.at[3 * z]))
        copies.append(pltpu.make_async_copy(blocks.at[z, pl.ds(rows, thin)], key.at[:, here], sems.at[3 * z + 1]))
        copies.append(pltpu.make_async_copy(blocks.at[z, pl.ds(rows + thin, thin)], value.at[:, here], sems.at[3 * z + 2]))
    for copy in copies:
        copy.start()
    tiles = f_query.shape[0]
    f_query[...] = factors[0:tiles, :]
    f_key[...] = factors[tiles : tiles + 1, 0:thin]
    f_value[...] = factors[tiles : tiles + 1, thin : 2 * thin]
    norm_out[...] = norm[...]
    for copy in copies:
        copy.wait()


def on_device(first_q, second_q, first_k, second_k, first_v, second_v, mix, train, step):
    n, m = lax.axis_size("zero"), lax.axis_size("model")
    rows, cols = first_q.shape
    thin = first_k.shape[1]
    wide = rows + 2 * thin
    piece = train.shape[0]
    tiles = rows // LANES
    f32, bf16 = jnp.float32, jnp.bfloat16
    anywhere = pl.BlockSpec(memory_space=pltpu.HBM)
    vmem = pl.BlockSpec(memory_space=pltpu.VMEM)
    dma = pltpu.SemaphoreType.DMA
    norm_rows = n * m * piece // LANES
    blocks, factors, norm = pl.pallas_call(
        gather_kernel,
        out_shape=(
            pltpu.VMEM((n, wide, cols), bf16),
            pltpu.VMEM((8, LANES), f32),
            pltpu.VMEM((norm_rows, LANES), bf16),
        ),
        in_specs=[anywhere] * 9,
        out_specs=(vmem, vmem, vmem),
        scratch_shapes=[
            pltpu.VMEM((rows, cols), f32),
            pltpu.VMEM((rows, cols), f32),
            pltpu.VMEM((2 * thin, rows), f32),
            pltpu.VMEM((2 * thin, rows), f32),
            pltpu.VMEM((1, rows), f32),
            pltpu.VMEM((rows, LANES), f32),
            pltpu.VMEM((2, 1, piece), f32),
            pltpu.VMEM((8, LANES), f32),
            pltpu.VMEM((wide, cols), f32),
            pltpu.VMEM((n, 8, LANES), f32),
            pltpu.VMEM((m, n, LANES), f32),
            pltpu.VMEM((norm_rows, LANES), f32),
            dma((1 + 2 * tiles + 6,)),
            dma((n,)),
            dma((n,)),
            dma((m,)),
            dma((m,)),
            dma((n // 2 * PIECES,)),
            dma((n // 2 * PIECES,)),
            dma((n // 2 * PIECES,)),
            dma((n // 2 * PIECES,)),
        ],
        compiler_params=pltpu.CompilerParams(
            collective_id=0, has_side_effects=True, vmem_limit_bytes=24 * 1024 * 1024
        ),
        name="gather",
    )(
        first_q, second_q, first_k.T, second_k.T, first_v.T, second_v.T,
        mix.reshape(1, rows), train.reshape(1, piece), step.reshape(1, piece),
    )
    query, key, value, f_query, f_key, f_value, norm = pl.pallas_call(
        functools.partial(place_kernel, n, rows, thin),
        out_shape=(
            jax.ShapeDtypeStruct((n * rows, cols), bf16),
            jax.ShapeDtypeStruct((thin, n * rows), bf16),
            jax.ShapeDtypeStruct((thin, n * rows), bf16),
            jax.ShapeDtypeStruct((tiles, LANES), f32),
            jax.ShapeDtypeStruct((1, thin), f32),
            jax.ShapeDtypeStruct((1, thin), f32),
            jax.ShapeDtypeStruct((norm_rows, LANES), bf16),
        ),
        in_specs=[vmem, vmem, vmem],
        out_specs=(anywhere, anywhere, anywhere, vmem, vmem, vmem, vmem),
        scratch_shapes=[dma((3 * n,))],
        compiler_params=pltpu.CompilerParams(vmem_limit_bytes=24 * 1024 * 1024),
        name="place",
    )(blocks, factors, norm)
    return (
        query, key.T, value.T,
        f_query.reshape(-1), f_key.reshape(-1), f_value.reshape(-1), norm.reshape(-1),
    )


def solution(mesh):
    own = P(("unit", "zero"), "model")
    return jax.shard_map(
        on_device,
        mesh=mesh,
        in_specs=(own, own, own, own, own, own, P(("unit", "zero")), P(("unit", "zero", "model")), P(("unit", "zero", "model"))),
        out_specs=(
            P("unit", "model"), P("unit", "model"), P("unit", "model"),
            P(("unit", "model")), P(("unit", "model")), P(("unit", "model")), P("unit"),
        ),
        check_vma=False,
    )
```

```python
import functools
import math

import jax
import jax.numpy as jnp
from jax import lax
from jax.experimental import pallas as pl
from jax.experimental.pallas import tpu as pltpu
from jax.sharding import PartitionSpec as P

MESH = pl.DeviceIdType.MESH
LANES = 128
PIECES = 8
EARLY = 1


def gather_kernel(
    first_q, second_q, first_k, second_k, first_v, second_v, mix, train, step,
    blocks, f_query, f_key, f_value, norm,
    a_q, b_q, a_kv, b_kv, mix_row, share, norm_in, lane_row, fresh, stat, gains, plane, norm_wide, early,
    load_sem, line_sem, plane_send, plane_recv, early_send, early_recv, sent_sem, right_recv, left_recv,
):
    n, m = lax.axis_size("zero"), lax.axis_size("model")
    me, col = lax.axis_index("zero"), lax.axis_index("model")
    rows, cols = first_q.shape
    thin = first_k.shape[0]
    wide = rows + 2 * thin
    size = wide // PIECES
    half = PIECES // 2
    tiles = rows // LANES
    side = math.isqrt(m)
    across, down = lax.rem(col, side), col // side

    def beside(d):
        return down * side + lax.rem(across + d, side)

    def below(d):
        return lax.rem(down + d, side) * side + across

    loads = [pltpu.make_async_copy(mix, mix_row, load_sem.at[0])]
    for r in range(tiles):
        part = pl.ds(r * LANES, LANES)
        loads.append(pltpu.make_async_copy(first_q.at[part], a_q.at[part], load_sem.at[1 + 2 * r]))
        loads.append(pltpu.make_async_copy(second_q.at[part], b_q.at[part], load_sem.at[2 + 2 * r]))
    at = 1 + 2 * tiles
    for k, (src, dst) in enumerate(
        (
            (first_k, a_kv.at[pl.ds(0, thin)]),
            (first_v, a_kv.at[pl.ds(thin, thin)]),
            (second_k, b_kv.at[pl.ds(0, thin)]),
            (second_v, b_kv.at[pl.ds(thin, thin)]),
            (train, norm_in.at[0]),
            (step, norm_in.at[1]),
        )
    ):
        loads.append(pltpu.make_async_copy(src, dst, load_sem.at[at + k]))
    for load in loads:
        load.start()

    barrier = pltpu.get_barrier_semaphore()

    def greet_line(d, c):
        pl.semaphore_signal(barrier, inc=1, device_id={"zero": lax.rem(me + d, n)}, device_id_type=MESH)
        return c

    lax.fori_loop(1, n, greet_line, 0)
    for peer in (beside(1), beside(side - 1), below(1), below(side - 1)):
        pl.semaphore_signal(barrier, inc=1, device_id={"model": peer}, device_id_type=MESH)

    loads[0].wait()
    for r in range(tiles):
        row = mix_row[:, r * LANES : (r + 1) * LANES]
        share[r * LANES : (r + 1) * LANES, :] = jnp.broadcast_to(row, (LANES, LANES)).T

    sums = [jnp.zeros((8, LANES), jnp.float32) for _ in range(tiles)]
    for r in range(tiles):
        loads[1 + 2 * r].wait()
        loads[2 + 2 * r].wait()
        part = slice(r * LANES, (r + 1) * LANES)
        w = share[part, :]
        for c in range(tiles):
            lanes = slice(c * LANES, (c + 1) * LANES)
            f = w * a_q[part, lanes] + (1.0 - w) * b_q[part, lanes]
            fresh[part, lanes] = f
            sums[c] = sums[c] + jnp.sum((f * f).reshape(LANES // 8, 8, LANES), axis=0)
    for load in loads[at : at + 4]:
        load.wait()
    w = mix_row[...]
    f = w * a_kv[...] + (1.0 - w) * b_kv[...]
    fresh[rows:, :] = f
    s = f * f
    folded = s[:, :LANES]
    for c in range(1, tiles):
        folded = folded + s[:, c * LANES : (c + 1) * LANES]
    thin_sum = jnp.sum(folded.T, axis=0, keepdims=True)

    for load in loads[at + 4 :]:
        load.wait()
    gain = (norm_in[0] + norm_in[1]).astype(jnp.bfloat16).astype(jnp.float32)
    lane_row[...] = jnp.zeros_like(lane_row)
    share_of_row = gain.shape[1]
    per_row = LANES // share_of_row
    lane_row[0:1, 0:share_of_row] = gain
    gain = lane_row[...]
    spread = gain
    for k in range(1, per_row):
        spread = spread + pltpu.roll(gain, k * share_of_row, 1)
    lane = lax.broadcasted_iota(jnp.int32, (8, LANES), 1)
    spread = jnp.where(lane // share_of_row == lax.rem(col, per_row), spread, 0.0)

    for c in range(tiles):
        stat[me, c] = jnp.sum(sums[c], axis=0, keepdims=True)
    stat[me, tiles] = thin_sum
    gains[me] = spread[0:1, :]

    pl.semaphore_wait(barrier, n - 1 + 4)

    def to_line(ref, k, d):
        return pltpu.make_async_remote_copy(
            ref.at[me], ref.at[me], line_sem.at[2 * k], line_sem.at[2 * k + 1],
            device_id={"zero": lax.rem(me + d, n)}, device_id_type=MESH,
        )

    def whole_line(ref, k):
        every = ref.at[pl.ds(0, n - 1)]
        return pltpu.make_async_remote_copy(
            every, every, line_sem.at[2 * k], line_sem.at[2 * k + 1],
            device_id={"zero": lax.rem(me + 1, n)}, device_id_type=MESH,
        )

    for k, ref in enumerate((stat, gains)):
        to_line(ref, k, n // 2).start()
        for d in range(1, n // 2):
            to_line(ref, k, n // 2 + d).start()
            to_line(ref, k, n // 2 - d).start()

    after, before = lax.rem(me + 1, n), lax.rem(me + n - 1, n)

    def early_copy(p, way):
        where = pl.ds(p * size, size)
        return pltpu.make_async_remote_copy(
            fresh.at[where], early.at[way, where], early_send.at[way * EARLY + p], early_recv.at[way * EARLY + p],
            device_id={"zero": (after, before)[way]}, device_id_type=MESH,
        )

    for p in range(EARLY):
        early_copy(p, 0).start()
        early_copy(p, 1).start()

    whole_line(stat, 0).wait_recv()

    inverse = []
    for c in range(tiles + 1):
        total = stat[0, c]
        for z in range(1, n):
            total = total + stat[z, c]
        factor = jnp.sqrt(total)
        inverse.append(1.0 / factor)
        if c < tiles:
            f_query[c : c + 1, :] = factor
        else:
            f_key[...] = factor[:, :thin]
            f_value[...] = factor[:, thin:]
    thin_inverse = jnp.broadcast_to(inverse[tiles], (LANES, LANES)).T

    def rounded(source, owner, p):
        base = pl.multiple_of(owner * wide, wide)
        low, high = p * size, (p + 1) * size
        edge = min(max(rows, low), high)
        if low < edge:
            for c in range(tiles):
                lanes = slice(c * LANES, (c + 1) * LANES)
                blocks[pl.ds(base + low, edge - low), lanes] = (source[low:edge, lanes] * inverse[c]).astype(jnp.bfloat16)
        if edge < high:
            scale = thin_inverse[edge - rows : high - rows, :]
            for c in range(tiles):
                lanes = slice(c * LANES, (c + 1) * LANES)
                blocks[pl.ds(base + edge, high - edge), lanes] = (source[edge:high, lanes] * scale).astype(jnp.bfloat16)

    def piece_copy(way, recv, origin, s, p, to):
        where = blocks.at[pl.ds(pl.multiple_of(origin * wide + p * size, size), size)]
        return pltpu.make_async_remote_copy(
            where, where, sent_sem.at[way], recv.at[s * PIECES + p],
            device_id={"zero": to}, device_id_type=MESH,
        )

    def to_right(s, p):
        return piece_copy(0, right_recv, lax.rem(me + n - s, n), s, p, after)

    def to_left(s, p):
        return piece_copy(1, left_recv, lax.rem(me + s, n), s, p, before)

    def from_left(s, p):
        return piece_copy(0, right_recv, lax.rem(before + n - s, n), s, p, after)

    def from_right(s, p):
        return piece_copy(1, left_recv, lax.rem(after + s, n), s, p, before)

    def both(s, p):
        to_right(s, p).start()
        to_left(s, p).start()

    for p in range(EARLY, PIECES):
        rounded(fresh, me, p)
        if p > EARLY:
            both(0, p - 1)
    for p in range(EARLY):
        rounded(fresh, me, p)
    both(0, PIECES - 1)
    for p in range(EARLY):
        early_copy(p, 0).wait_recv()
        rounded(early.at[0], before, p)
        if p:
            to_left(1, p - 1).start()
        early_copy(p, 1).wait_recv()
        rounded(early.at[1], after, p)
        to_right(1, p).start()

    whole_line(gains, 1).wait_recv()
    for z in range(n):
        plane[col, z : z + 1, :] = gains[z]
    if EARLY:
        to_left(1, EARLY - 1).start()

    def plane_copy(k):
        if k < side - 1:
            slot = plane.at[pl.ds(beside(side - k), 1)]
            to = beside(1)
        else:
            slot = plane.at[pl.ds(lax.rem(down + side - (k - side + 1), side) * side, side)]
            to = below(1)
        return pltpu.make_async_remote_copy(
            slot, slot, plane_send.at[k], plane_recv.at[k], device_id={"model": to}, device_id_type=MESH
        )

    def plane_from(k):
        if k < side - 1:
            slot = plane.at[pl.ds(beside(2 * side - 1 - k), 1)]
            to = beside(1)
        else:
            slot = plane.at[pl.ds(lax.rem(down + 2 * side - 1 - (k - side + 1), side) * side, side)]
            to = below(1)
        return pltpu.make_async_remote_copy(
            slot, slot, plane_send.at[k], plane_recv.at[k], device_id={"model": to}, device_id_type=MESH
        )

    last = n // 2 - 1
    turns = 2 * (side - 1)
    plane_copy(0).start()
    for s in range(1, last):

        def one(p, c):
            from_left(s - 1, p).wait_recv()
            to_right(s, p).start()
            from_right(s - 1, p).wait_recv()
            to_left(s, p).start()
            return c

        lax.fori_loop(EARLY if s == 1 else 0, PIECES, one, 0)
        if s <= turns:
            plane_from(s - 1).wait_recv()
            if s < turns:
                plane_copy(s).start()
    for k in range(max(last - 1, 0), turns):
        plane_from(k).wait_recv()
        if k + 1 < turns:
            plane_copy(k + 1).start()

    per = m // per_row
    for k in range(per):
        line = plane[k * per_row]
        for j in range(1, per_row):
            line = line + plane[k * per_row + j]
        norm_wide[pl.ds(k, n, stride=per), :] = line
    norm[...] = norm_wide[...].astype(jnp.bfloat16)

    def near(p, c):
        from_left(last - 1, p).wait_recv()
        to_right(last, p).start()
        from_right(last - 1, p + half).wait_recv()
        to_left(last, p + half).start()
        return c

    def far(p, c):
        from_right(last - 1, p).wait_recv()
        from_left(last - 1, p + half).wait_recv()
        return c

    def end(p, c):
        from_left(last, p).wait_recv()
        from_right(last, p + half).wait_recv()
        return c

    lax.fori_loop(0, half, near, 0)
    lax.fori_loop(0, half, far, 0)
    lax.fori_loop(0, half, end, 0)

    for p in range(EARLY):
        early_copy(p, 0).wait_send()
        early_copy(p, 1).wait_send()
    out = blocks.at[pl.ds(0, (last * PIECES - EARLY + half) * size)]
    for way, to in enumerate((after, before)):
        pltpu.make_async_remote_copy(
            out, out, sent_sem.at[way], right_recv.at[0], device_id={"zero": to}, device_id_type=MESH
        ).wait_send()
    whole_line(stat, 0).wait_send()
    whole_line(gains, 1).wait_send()
    for k in range(turns):
        plane_copy(k).wait_send()


def place_kernel(n, rows, thin, blocks, *refs):
    query, key, value = refs[4:7]
    sems = refs[-1]
    wide = rows + 2 * thin
    pairs = []
    for z in range(n):
        here = pl.ds(z * rows, rows)
        pairs.append((blocks.at[pl.ds(z * wide, rows)], query.at[here]))
        pairs.append((blocks.at[pl.ds(z * wide + rows, thin)], key.at[:, here]))
        pairs.append((blocks.at[pl.ds(z * wide + rows + thin, thin)], value.at[:, here]))
    pairs.extend(zip(refs[:4], refs[7:11]))
    copies = [pltpu.make_async_copy(src, dst, sems.at[k]) for k, (src, dst) in enumerate(pairs)]
    for copy in copies:
        copy.start()
    for copy in copies:
        copy.wait()


def on_device(first_q, second_q, first_k, second_k, first_v, second_v, mix, train, step):
    n, m = lax.axis_size("zero"), lax.axis_size("model")
    rows, cols = first_q.shape
    thin = first_k.shape[1]
    wide = rows + 2 * thin
    piece = train.shape[0]
    tiles = rows // LANES
    f32, bf16 = jnp.float32, jnp.bfloat16
    anywhere = pl.BlockSpec(memory_space=pltpu.HBM)
    vmem = pl.BlockSpec(memory_space=pltpu.VMEM)
    dma = pltpu.SemaphoreType.DMA
    norm_rows = n * m * piece // LANES
    hbm = lambda x: pltpu.with_memory_space_constraint(x, pltpu.HBM)
    blocks, *small = pl.pallas_call(
        gather_kernel,
        out_shape=(
            pltpu.VMEM((n * wide, cols), bf16),
            pltpu.VMEM((tiles, LANES), f32),
            pltpu.VMEM((1, thin), f32),
            pltpu.VMEM((1, thin), f32),
            pltpu.VMEM((norm_rows, LANES), bf16),
        ),
        in_specs=[anywhere] * 9,
        out_specs=(vmem,) * 5,
        scratch_shapes=[
            pltpu.VMEM((rows, cols), f32),
            pltpu.VMEM((rows, cols), f32),
            pltpu.VMEM((2 * thin, rows), f32),
            pltpu.VMEM((2 * thin, rows), f32),
            pltpu.VMEM((1, rows), f32),
            pltpu.VMEM((rows, LANES), f32),
            pltpu.VMEM((2, 1, piece), f32),
            pltpu.VMEM((8, LANES), f32),
            pltpu.VMEM((wide, cols), f32),
            pltpu.VMEM((n, tiles + 1, 1, LANES), f32),
            pltpu.VMEM((n, 1, LANES), f32),
            pltpu.VMEM((m, n, LANES), f32),
            pltpu.VMEM((norm_rows, LANES), f32),
            pltpu.VMEM((2, max(EARLY, 1) * wide // PIECES, cols), f32),
            dma((1 + 2 * tiles + 6,)),
            dma((4,)),
            dma((2 * (math.isqrt(m) - 1),)),
            dma((2 * (math.isqrt(m) - 1),)),
            dma((2 * max(EARLY, 1),)),
            dma((2 * max(EARLY, 1),)),
            dma((2,)),
            dma((n // 2 * PIECES,)),
            dma((n // 2 * PIECES,)),
        ],
        compiler_params=pltpu.CompilerParams(
            collective_id=0, has_side_effects=True, vmem_limit_bytes=24 * 1024 * 1024
        ),
        name="gather",
    )(
        hbm(first_q), hbm(second_q), hbm(first_k.T), hbm(second_k.T), hbm(first_v.T), hbm(second_v.T),
        hbm(mix.reshape(1, rows)), hbm(train.reshape(1, piece)), hbm(step.reshape(1, piece)),
    )
    query, key, value, f_query, f_key, f_value, norm = pl.pallas_call(
        functools.partial(place_kernel, n, rows, thin),
        out_shape=(
            jax.ShapeDtypeStruct((n * rows, cols), bf16),
            jax.ShapeDtypeStruct((thin, n * rows), bf16),
            jax.ShapeDtypeStruct((thin, n * rows), bf16),
            jax.ShapeDtypeStruct((tiles, LANES), f32),
            jax.ShapeDtypeStruct((1, thin), f32),
            jax.ShapeDtypeStruct((1, thin), f32),
            jax.ShapeDtypeStruct((norm_rows, LANES), bf16),
        ),
        in_specs=[vmem] * 5,
        out_specs=(anywhere,) * 7,
        scratch_shapes=[dma((3 * n + 4,))],
        compiler_params=pltpu.CompilerParams(vmem_limit_bytes=24 * 1024 * 1024),
        name="place",
    )(blocks, *small)
    return (
        query, key.T, value.T,
        f_query.reshape(-1), f_key.reshape(-1), f_value.reshape(-1), norm.reshape(-1),
    )


def solution(mesh):
    own = P(("unit", "zero"), "model")
    return jax.shard_map(
        on_device,
        mesh=mesh,
        in_specs=(own, own, own, own, own, own, P(("unit", "zero")), P(("unit", "zero", "model")), P(("unit", "zero", "model"))),
        out_specs=(
            P("unit", "model"), P("unit", "model"), P("unit", "model"),
            P(("unit", "model")), P(("unit", "model")), P(("unit", "model")), P("unit"),
        ),
        check_vma=False,
    )
```

```python
import functools
import math

import jax
import jax.numpy as jnp
from jax import lax
from jax.experimental import pallas as pl
from jax.experimental.pallas import tpu as pltpu
from jax.sharding import PartitionSpec as P

MESH = pl.DeviceIdType.MESH
LANES = 128
PIECES = 4
EARLY = 80


def gather_kernel(
    first_q, second_q, first_k, second_k, first_v, second_v, mix, train, step,
    blocks, f_query, f_key, f_value, norm,
    a_q, b_q, a_kv, b_kv, mix_row, share, norm_in, lane_row, fresh, stat, gains, plane, norm_wide, early,
    load_sem, line_sem, plane_send, plane_recv, early_send, early_recv, sent_sem, right_recv, left_recv,
):
    n, m = lax.axis_size("zero"), lax.axis_size("model")
    me, col = lax.axis_index("zero"), lax.axis_index("model")
    rows, cols = first_q.shape
    thin = first_k.shape[0]
    wide = rows + 2 * thin
    size = wide // PIECES
    half = PIECES // 2
    tiles = rows // LANES
    side = math.isqrt(m)
    across, down = lax.rem(col, side), col // side

    def beside(d):
        return down * side + lax.rem(across + d, side)

    def below(d):
        return lax.rem(down + d, side) * side + across

    def load(k, src, dst):
        return pltpu.make_async_copy(src, dst, load_sem.at[k])

    load_mix = load(0, mix, mix_row)
    load_thin = [
        load(1, first_k, a_kv.at[pl.ds(0, thin)]),
        load(2, second_k, b_kv.at[pl.ds(0, thin)]),
        load(3, first_v, a_kv.at[pl.ds(thin, thin)]),
        load(4, second_v, b_kv.at[pl.ds(thin, thin)]),
    ]
    load_gain = [load(5, train, norm_in.at[0]), load(6, step, norm_in.at[1])]
    load_q = []
    for r in range(tiles):
        part = pl.ds(r * LANES, LANES)
        load_q.append(
            (load(7 + 2 * r, first_q.at[part], a_q.at[part]), load(8 + 2 * r, second_q.at[part], b_q.at[part]))
        )

    def around(d):
        return {"zero": lax.rem(me + d, n)}

    barrier = pltpu.get_barrier_semaphore()

    outward = [n // 2]
    for d in range(n // 2 - 1, 0, -1):
        outward += [d, n - d]
    for d in outward:
        pl.semaphore_signal(barrier, inc=1, device_id=around(d), device_id_type=MESH)
    for peer in (beside(1), beside(side - 1), below(1), below(side - 1)):
        pl.semaphore_signal(barrier, inc=1, device_id={"model": peer}, device_id_type=MESH)
    load_mix.start()
    for copy in load_thin:
        copy.start()
    for pair in load_q:
        for copy in pair:
            copy.start()
    for copy in load_gain:
        copy.start()

    load_mix.wait()
    for r in range(tiles):
        row = mix_row[:, r * LANES : (r + 1) * LANES]
        share[r * LANES : (r + 1) * LANES, :] = jnp.broadcast_to(row, (LANES, LANES)).T

    sums = [jnp.zeros((8, LANES), jnp.float32) for _ in range(tiles)]
    for r in range(tiles):
        if r == tiles - 1:
            for copy in load_thin:
                copy.wait()
            w = mix_row[...]
            f = w * a_kv[...] + (1.0 - w) * b_kv[...]
            fresh[rows:, :] = f
            s = f * f
            folded = s[:, :LANES]
            for c in range(1, tiles):
                folded = folded + s[:, c * LANES : (c + 1) * LANES]
            stat[me, tiles] = jnp.sum(folded.T, axis=0, keepdims=True)
        for copy in load_q[r]:
            copy.wait()
        part = slice(r * LANES, (r + 1) * LANES)
        w = share[part, :]
        for c in range(tiles):
            lanes = slice(c * LANES, (c + 1) * LANES)
            f = w * a_q[part, lanes] + (1.0 - w) * b_q[part, lanes]
            fresh[part, lanes] = f
            sums[c] = sums[c] + jnp.sum((f * f).reshape(LANES // 8, 8, LANES), axis=0)
    for c in range(tiles):
        stat[me, c] = jnp.sum(sums[c], axis=0, keepdims=True)

    pl.semaphore_wait(barrier, n - 1 + 4)

    def to_line(ref, k, d):
        return pltpu.make_async_remote_copy(
            ref.at[me], ref.at[me], line_sem.at[2 * k], line_sem.at[2 * k + 1],
            device_id=around(d), device_id_type=MESH,
        )

    def whole_line(ref, k):
        every = ref.at[pl.ds(0, n - 1)]
        return pltpu.make_async_remote_copy(
            every, every, line_sem.at[2 * k], line_sem.at[2 * k + 1],
            device_id={"zero": lax.rem(me + 1, n)}, device_id_type=MESH,
        )

    for d in outward:
        to_line(stat, 0, d).start()

    after, before = lax.rem(me + 1, n), lax.rem(me + n - 1, n)

    def early_copy(way):
        return pltpu.make_async_remote_copy(
            fresh.at[pl.ds(0, EARLY)], early.at[way], early_send.at[way], early_recv.at[way],
            device_id={"zero": (after, before)[way]}, device_id_type=MESH,
        )

    ways = (0, 1) if EARLY else ()
    for way in ways:
        early_copy(way).start()

    for copy in load_gain:
        copy.wait()
    gain = (norm_in[0] + norm_in[1]).astype(jnp.bfloat16).astype(jnp.float32)
    lane_row[...] = jnp.zeros_like(lane_row)
    share_of_row = gain.shape[1]
    per_row = LANES // share_of_row
    lane_row[0:1, 0:share_of_row] = gain
    gain = lane_row[...]
    spread = gain
    for k in range(1, per_row):
        spread = spread + pltpu.roll(gain, k * share_of_row, 1)
    lane = lax.broadcasted_iota(jnp.int32, (8, LANES), 1)
    spread = jnp.where(lane // share_of_row == lax.rem(col, per_row), spread, 0.0)

    gains[me] = spread[0:1, :]
    for d in outward:
        to_line(gains, 1, d).start()

    whole_line(stat, 0).wait_recv()

    inverse = []
    for c in range(tiles + 1):
        total = stat[0, c]
        for z in range(1, n):
            total = total + stat[z, c]
        factor = jnp.sqrt(total)
        inverse.append(1.0 / factor)
        if c < tiles:
            f_query[c : c + 1, :] = factor
        else:
            f_key[...] = factor[:, :thin]
            f_value[...] = factor[:, thin:]
    thin_inverse = jnp.broadcast_to(inverse[tiles], (LANES, LANES)).T

    def rounded(source, owner, low, high):
        base = pl.multiple_of(owner * wide, wide)
        edge = min(max(rows, low), high)
        if low < edge:
            for c in range(tiles):
                lanes = slice(c * LANES, (c + 1) * LANES)
                blocks[pl.ds(base + low, edge - low), lanes] = (source[low:edge, lanes] * inverse[c]).astype(jnp.bfloat16)
        if edge < high:
            scale = thin_inverse[edge - rows : high - rows, :]
            for c in range(tiles):
                lanes = slice(c * LANES, (c + 1) * LANES)
                blocks[pl.ds(base + edge, high - edge), lanes] = (source[edge:high, lanes] * scale).astype(jnp.bfloat16)

    def piece_copy(way, recv, origin, s, p, to):
        skip = EARLY if s == 0 and p == 0 else 0
        start = pl.multiple_of(origin * wide + p * size + skip, 16)
        where = blocks.at[pl.ds(start, size - skip)]
        return pltpu.make_async_remote_copy(
            where, where, sent_sem.at[way], recv.at[s * PIECES + p],
            device_id={"zero": to}, device_id_type=MESH,
        )

    def to_right(s, p):
        return piece_copy(0, right_recv, lax.rem(me + n - s, n), s, p, after)

    def to_left(s, p):
        return piece_copy(1, left_recv, lax.rem(me + s, n), s, p, before)

    def from_left(s, p):
        return piece_copy(0, right_recv, lax.rem(before + n - s, n), s, p, after)

    def from_right(s, p):
        return piece_copy(1, left_recv, lax.rem(after + s, n), s, p, before)

    for p in range(PIECES):
        rounded(fresh, me, p * size if p else EARLY, (p + 1) * size)
        if p:
            to_right(0, p - 1).start()
            to_left(0, p - 1).start()
    if EARLY:
        rounded(fresh, me, 0, EARLY)
    to_right(0, PIECES - 1).start()
    to_left(0, PIECES - 1).start()
    for way in ways:
        early_copy(way).wait_recv()
        rounded(early.at[way], (before, after)[way], 0, EARLY)

    whole_line(gains, 1).wait_recv()
    for z in range(n):
        plane[col, z : z + 1, :] = gains[z]

    def plane_copy(k):
        if k < side - 1:
            slot = plane.at[pl.ds(beside(side - k), 1)]
            to = beside(1)
        else:
            slot = plane.at[pl.ds(lax.rem(down + side - (k - side + 1), side) * side, side)]
            to = below(1)
        return pltpu.make_async_remote_copy(
            slot, slot, plane_send.at[k], plane_recv.at[k], device_id={"model": to}, device_id_type=MESH
        )

    def plane_from(k):
        if k < side - 1:
            slot = plane.at[pl.ds(beside(2 * side - 1 - k), 1)]
            to = beside(1)
        else:
            slot = plane.at[pl.ds(lax.rem(down + 2 * side - 1 - (k - side + 1), side) * side, side)]
            to = below(1)
        return pltpu.make_async_remote_copy(
            slot, slot, plane_send.at[k], plane_recv.at[k], device_id={"model": to}, device_id_type=MESH
        )

    last = n // 2 - 1
    turns = 2 * (side - 1)
    plane_copy(0).start()
    for s in range(1, last):

        def one(p, c):
            from_left(s - 1, p).wait_recv()
            to_right(s, p).start()
            from_right(s - 1, p).wait_recv()
            to_left(s, p).start()
            return c

        for p in range(PIECES):
            one(p, 0)
        if s <= turns:
            plane_from(s - 1).wait_recv()
            if s < turns:
                plane_copy(s).start()
    for k in range(max(last - 1, 0), turns):
        plane_from(k).wait_recv()
        if k + 1 < turns:
            plane_copy(k + 1).start()

    per = m // per_row
    for k in range(per):
        line = plane[k * per_row]
        for j in range(1, per_row):
            line = line + plane[k * per_row + j]
        norm_wide[pl.ds(k, n, stride=per), :] = line
    norm[...] = norm_wide[...].astype(jnp.bfloat16)

    def near(p, c):
        from_left(last - 1, p).wait_recv()
        to_right(last, p).start()
        from_right(last - 1, p + half).wait_recv()
        to_left(last, p + half).start()
        return c

    def far(p, c):
        from_right(last - 1, p).wait_recv()
        from_left(last - 1, p + half).wait_recv()
        return c

    def end(p, c):
        from_left(last, p).wait_recv()
        from_right(last, p + half).wait_recv()
        return c

    lax.fori_loop(0, half, near, 0)
    lax.fori_loop(0, half, far, 0)
    lax.fori_loop(0, half, end, 0)

    for way in ways:
        early_copy(way).wait_send()
    out = blocks.at[pl.ds(0, (last * PIECES + half) * size - EARLY)]
    for way, to in enumerate((after, before)):
        pltpu.make_async_remote_copy(
            out, out, sent_sem.at[way], right_recv.at[0], device_id={"zero": to}, device_id_type=MESH
        ).wait_send()
    whole_line(stat, 0).wait_send()
    whole_line(gains, 1).wait_send()
    for k in range(turns):
        plane_copy(k).wait_send()


def place_kernel(n, rows, thin, blocks, *refs):
    query, key, value = refs[4:7]
    sems = refs[-1]
    wide = rows + 2 * thin
    for z in range(n):
        here = pl.ds(z * rows, rows)
        pltpu.make_async_copy(blocks.at[pl.ds(z * wide, rows)], query.at[here], sems.at[0]).start()
        pltpu.make_async_copy(blocks.at[pl.ds(z * wide + rows, thin)], key.at[:, here], sems.at[1]).start()
        pltpu.make_async_copy(blocks.at[pl.ds(z * wide + rows + thin, thin)], value.at[:, here], sems.at[2]).start()
    small = [
        pltpu.make_async_copy(src, dst, sems.at[3 + k]) for k, (src, dst) in enumerate(zip(refs[:4], refs[7:11]))
    ]
    for copy in small:
        copy.start()
    for copy in small:
        copy.wait()
    for k, large in enumerate((query, key, value)):
        pltpu.make_async_copy(large, large, sems.at[k]).wait()


def on_device(first_q, second_q, first_k, second_k, first_v, second_v, mix, train, step):
    n, m = lax.axis_size("zero"), lax.axis_size("model")
    rows, cols = first_q.shape
    thin = first_k.shape[1]
    wide = rows + 2 * thin
    piece = train.shape[0]
    tiles = rows // LANES
    f32, bf16 = jnp.float32, jnp.bfloat16
    anywhere = pl.BlockSpec(memory_space=pltpu.HBM)
    vmem = pl.BlockSpec(memory_space=pltpu.VMEM)
    dma = pltpu.SemaphoreType.DMA
    norm_rows = n * m * piece // LANES
    hbm = lambda x: pltpu.with_memory_space_constraint(x, pltpu.HBM)
    blocks, *small = pl.pallas_call(
        gather_kernel,
        out_shape=(
            pltpu.VMEM((n * wide, cols), bf16),
            pltpu.VMEM((tiles, LANES), f32),
            pltpu.VMEM((1, thin), f32),
            pltpu.VMEM((1, thin), f32),
            pltpu.VMEM((norm_rows, LANES), bf16),
        ),
        in_specs=[anywhere] * 9,
        out_specs=(vmem,) * 5,
        scratch_shapes=[
            pltpu.VMEM((rows, cols), f32),
            pltpu.VMEM((rows, cols), f32),
            pltpu.VMEM((2 * thin, rows), f32),
            pltpu.VMEM((2 * thin, rows), f32),
            pltpu.VMEM((1, rows), f32),
            pltpu.VMEM((rows, LANES), f32),
            pltpu.VMEM((2, 1, piece), f32),
            pltpu.VMEM((8, LANES), f32),
            pltpu.VMEM((wide, cols), f32),
            pltpu.VMEM((n, tiles + 1, 1, LANES), f32),
            pltpu.VMEM((n, 1, LANES), f32),
            pltpu.VMEM((m, n, LANES), f32),
            pltpu.VMEM((norm_rows, LANES), f32),
            pltpu.VMEM((2, max(EARLY, 8), cols), f32),
            dma((7 + 2 * tiles,)),
            dma((4,)),
            dma((2 * (math.isqrt(m) - 1),)),
            dma((2 * (math.isqrt(m) - 1),)),
            dma((2,)),
            dma((2,)),
            dma((2,)),
            dma((n // 2 * PIECES,)),
            dma((n // 2 * PIECES,)),
        ],
        compiler_params=pltpu.CompilerParams(
            collective_id=0, has_side_effects=True, vmem_limit_bytes=24 * 1024 * 1024
        ),
        name="gather",
    )(
        hbm(first_q), hbm(second_q), hbm(first_k.T), hbm(second_k.T), hbm(first_v.T), hbm(second_v.T),
        hbm(mix.reshape(1, rows)), hbm(train.reshape(1, piece)), hbm(step.reshape(1, piece)),
    )
    query, key, value, f_query, f_key, f_value, norm = pl.pallas_call(
        functools.partial(place_kernel, n, rows, thin),
        out_shape=(
            jax.ShapeDtypeStruct((n * rows, cols), bf16),
            jax.ShapeDtypeStruct((thin, n * rows), bf16),
            jax.ShapeDtypeStruct((thin, n * rows), bf16),
            jax.ShapeDtypeStruct((tiles, LANES), f32),
            jax.ShapeDtypeStruct((1, thin), f32),
            jax.ShapeDtypeStruct((1, thin), f32),
            jax.ShapeDtypeStruct((norm_rows, LANES), bf16),
        ),
        in_specs=[vmem] * 5,
        out_specs=(anywhere,) * 7,
        scratch_shapes=[dma((7,))],
        compiler_params=pltpu.CompilerParams(vmem_limit_bytes=24 * 1024 * 1024),
        name="place",
    )(blocks, *small)
    return (
        query, key.T, value.T,
        f_query.reshape(-1), f_key.reshape(-1), f_value.reshape(-1), norm.reshape(-1),
    )


def solution(mesh):
    own = P(("unit", "zero"), "model")
    return jax.shard_map(
        on_device,
        mesh=mesh,
        in_specs=(own, own, own, own, own, own, P(("unit", "zero")), P(("unit", "zero", "model")), P(("unit", "zero", "model"))),
        out_specs=(
            P("unit", "model"), P("unit", "model"), P("unit", "model"),
            P(("unit", "model")), P(("unit", "model")), P(("unit", "model")), P("unit"),
        ),
        check_vma=False,
    )
```

```python
import functools
import math

import jax
import jax.numpy as jnp
from jax import lax
from jax.experimental import pallas as pl
from jax.experimental.pallas import tpu as pltpu
from jax.sharding import PartitionSpec as P

MESH = pl.DeviceIdType.MESH
LANES = 128
PIECES = 4
EARLY = 96


def gather_kernel(
    first_q, second_q, first_k, second_k, first_v, second_v, mix, train, step,
    blocks, f_query, f_key, f_value, norm,
    a_q, b_q, a_kv, b_kv, mix_row, share, norm_in, lane_row, fresh, stat, plane, norm_wide, early,
    load_sem, line_sem, plane_send, plane_recv, early_send, early_recv, sent_sem, right_recv, left_recv,
):
    n, m = lax.axis_size("zero"), lax.axis_size("model")
    me, col = lax.axis_index("zero"), lax.axis_index("model")
    rows, cols = first_q.shape
    thin = first_k.shape[0]
    wide = rows + 2 * thin
    size = wide // PIECES
    half = PIECES // 2
    tiles = rows // LANES
    side = math.isqrt(m)
    across, down = lax.rem(col, side), col // side

    def beside(d):
        return down * side + lax.rem(across + d, side)

    def below(d):
        return lax.rem(down + d, side) * side + across

    def load(k, src, dst):
        return pltpu.make_async_copy(src, dst, load_sem.at[k])

    load_mix = load(0, mix, mix_row)
    load_thin = [
        load(1, first_k, a_kv.at[pl.ds(0, thin)]),
        load(2, second_k, b_kv.at[pl.ds(0, thin)]),
        load(3, first_v, a_kv.at[pl.ds(thin, thin)]),
        load(4, second_v, b_kv.at[pl.ds(thin, thin)]),
    ]
    load_gain = [load(5, train, norm_in.at[0]), load(6, step, norm_in.at[1])]
    load_q = []
    for r in range(tiles):
        part = pl.ds(r * LANES, LANES)
        load_q.append(
            (load(7 + 2 * r, first_q.at[part], a_q.at[part]), load(8 + 2 * r, second_q.at[part], b_q.at[part]))
        )

    def around(d):
        return {"zero": lax.rem(me + d, n)}

    barrier = pltpu.get_barrier_semaphore()

    outward = [n // 2]
    for d in range(n // 2 - 1, 0, -1):
        outward += [d, n - d]
    for d in outward:
        pl.semaphore_signal(barrier, inc=1, device_id=around(d), device_id_type=MESH)
    for peer in (beside(1), beside(side - 1), below(1), below(side - 1)):
        pl.semaphore_signal(barrier, inc=1, device_id={"model": peer}, device_id_type=MESH)
    load_mix.start()
    for copy in load_thin:
        copy.start()
    for pair in load_q:
        for copy in pair:
            copy.start()
    for copy in load_gain:
        copy.start()

    load_mix.wait()
    for r in range(tiles):
        row = mix_row[:, r * LANES : (r + 1) * LANES]
        share[r * LANES : (r + 1) * LANES, :] = jnp.broadcast_to(row, (LANES, LANES)).T

    sums = [jnp.zeros((8, LANES), jnp.float32) for _ in range(tiles)]
    for r in range(tiles):
        if r == tiles - 1:
            for copy in load_thin:
                copy.wait()
            w = mix_row[...]
            f = w * a_kv[...] + (1.0 - w) * b_kv[...]
            fresh[rows:, :] = f
            s = f * f
            folded = s[:, :LANES]
            for c in range(1, tiles):
                folded = folded + s[:, c * LANES : (c + 1) * LANES]
            stat[me, tiles] = jnp.sum(folded.T, axis=0, keepdims=True)
        for copy in load_q[r]:
            copy.wait()
        part = slice(r * LANES, (r + 1) * LANES)
        w = share[part, :]
        for c in range(tiles):
            lanes = slice(c * LANES, (c + 1) * LANES)
            f = w * a_q[part, lanes] + (1.0 - w) * b_q[part, lanes]
            fresh[part, lanes] = f
            sums[c] = sums[c] + jnp.sum((f * f).reshape(LANES // 8, 8, LANES), axis=0)
    for c in range(tiles):
        stat[me, c] = jnp.sum(sums[c], axis=0, keepdims=True)

    for copy in load_gain:
        copy.wait()
    gain = (norm_in[0] + norm_in[1]).astype(jnp.bfloat16).astype(jnp.float32)
    lane_row[...] = jnp.zeros_like(lane_row)
    share_of_row = gain.shape[1]
    per_row = LANES // share_of_row
    lane_row[0:1, 0:share_of_row] = gain
    gain = lane_row[...]
    spread = gain
    for k in range(1, per_row):
        spread = spread + pltpu.roll(gain, k * share_of_row, 1)
    lane = lax.broadcasted_iota(jnp.int32, (8, LANES), 1)
    spread = jnp.where(lane // share_of_row == lax.rem(col, per_row), spread, 0.0)

    stat[me, tiles + 1] = spread[0:1, :]

    pl.semaphore_wait(barrier, n - 1 + 4)

    def to_line(d):
        return pltpu.make_async_remote_copy(
            stat.at[me], stat.at[me], line_sem.at[0], line_sem.at[1], device_id=around(d), device_id_type=MESH
        )

    def whole_line():
        every = stat.at[pl.ds(0, n - 1)]
        return pltpu.make_async_remote_copy(
            every, every, line_sem.at[0], line_sem.at[1], device_id=around(1), device_id_type=MESH
        )

    for d in outward:
        to_line(d).start()

    after, before = lax.rem(me + 1, n), lax.rem(me + n - 1, n)

    def early_copy(way):
        return pltpu.make_async_remote_copy(
            fresh.at[pl.ds(0, EARLY)], early.at[way], early_send.at[way], early_recv.at[way],
            device_id={"zero": (after, before)[way]}, device_id_type=MESH,
        )

    ways = (0, 1) if EARLY else ()
    for way in ways:
        early_copy(way).start()

    whole_line().wait_recv()

    inverse = []
    for c in range(tiles + 1):
        total = stat[0, c]
        for z in range(1, n):
            total = total + stat[z, c]
        factor = jnp.sqrt(total)
        inverse.append(1.0 / factor)
        if c < tiles:
            f_query[c : c + 1, :] = factor
        else:
            f_key[...] = factor[:, :thin]
            f_value[...] = factor[:, thin:]
    thin_inverse = jnp.broadcast_to(inverse[tiles], (LANES, LANES)).T

    def rounded(source, owner, low, high):
        base = pl.multiple_of(owner * wide, wide)
        edge = min(max(rows, low), high)
        if low < edge:
            for c in range(tiles):
                lanes = slice(c * LANES, (c + 1) * LANES)
                blocks[pl.ds(base + low, edge - low), lanes] = (source[low:edge, lanes] * inverse[c]).astype(jnp.bfloat16)
        if edge < high:
            scale = thin_inverse[edge - rows : high - rows, :]
            for c in range(tiles):
                lanes = slice(c * LANES, (c + 1) * LANES)
                blocks[pl.ds(base + edge, high - edge), lanes] = (source[edge:high, lanes] * scale).astype(jnp.bfloat16)

    def piece_copy(way, recv, origin, s, p, to):
        skip = EARLY if s == 0 and p == 0 else 0
        start = pl.multiple_of(origin * wide + p * size + skip, 16)
        where = blocks.at[pl.ds(start, size - skip)]
        return pltpu.make_async_remote_copy(
            where, where, sent_sem.at[way], recv.at[s * PIECES + p],
            device_id={"zero": to}, device_id_type=MESH,
        )

    def to_right(s, p):
        return piece_copy(0, right_recv, lax.rem(me + n - s, n), s, p, after)

    def to_left(s, p):
        return piece_copy(1, left_recv, lax.rem(me + s, n), s, p, before)

    def from_left(s, p):
        return piece_copy(0, right_recv, lax.rem(before + n - s, n), s, p, after)

    def from_right(s, p):
        return piece_copy(1, left_recv, lax.rem(after + s, n), s, p, before)

    for p in range(PIECES):
        rounded(fresh, me, p * size if p else EARLY, (p + 1) * size)
        if p:
            to_right(0, p - 1).start()
            to_left(0, p - 1).start()
    if EARLY:
        rounded(fresh, me, 0, EARLY)
    to_right(0, PIECES - 1).start()
    to_left(0, PIECES - 1).start()
    for way in ways:
        early_copy(way).wait_recv()
        rounded(early.at[way], (before, after)[way], 0, EARLY)

    for z in range(n):
        plane[col, z : z + 1, :] = stat[z, tiles + 1]

    def plane_copy(k):
        if k < side - 1:
            slot = plane.at[pl.ds(beside(side - k), 1)]
            to = beside(1)
        else:
            slot = plane.at[pl.ds(lax.rem(down + side - (k - side + 1), side) * side, side)]
            to = below(1)
        return pltpu.make_async_remote_copy(
            slot, slot, plane_send.at[k], plane_recv.at[k], device_id={"model": to}, device_id_type=MESH
        )

    def plane_from(k):
        if k < side - 1:
            slot = plane.at[pl.ds(beside(2 * side - 1 - k), 1)]
            to = beside(1)
        else:
            slot = plane.at[pl.ds(lax.rem(down + 2 * side - 1 - (k - side + 1), side) * side, side)]
            to = below(1)
        return pltpu.make_async_remote_copy(
            slot, slot, plane_send.at[k], plane_recv.at[k], device_id={"model": to}, device_id_type=MESH
        )

    last = n // 2 - 1
    turns = 2 * (side - 1)
    plane_copy(0).start()
    for s in range(1, last):

        def one(p, c):
            from_left(s - 1, p).wait_recv()
            to_right(s, p).start()
            from_right(s - 1, p).wait_recv()
            to_left(s, p).start()
            return c

        for p in range(PIECES):
            one(p, 0)
        if s <= turns:
            plane_from(s - 1).wait_recv()
            if s < turns:
                plane_copy(s).start()
    for k in range(max(last - 1, 0), turns):
        plane_from(k).wait_recv()
        if k + 1 < turns:
            plane_copy(k + 1).start()

    per = m // per_row
    for k in range(per):
        line = plane[k * per_row]
        for j in range(1, per_row):
            line = line + plane[k * per_row + j]
        norm_wide[pl.ds(k, n, stride=per), :] = line
    norm[...] = norm_wide[...].astype(jnp.bfloat16)

    def near(p, c):
        from_left(last - 1, p).wait_recv()
        to_right(last, p).start()
        from_right(last - 1, p + half).wait_recv()
        to_left(last, p + half).start()
        return c

    def far(p, c):
        from_right(last - 1, p).wait_recv()
        from_left(last - 1, p + half).wait_recv()
        return c

    def end(p, c):
        from_left(last, p).wait_recv()
        from_right(last, p + half).wait_recv()
        return c

    lax.fori_loop(0, half, near, 0)
    lax.fori_loop(0, half, far, 0)
    lax.fori_loop(0, half, end, 0)

    for way in ways:
        early_copy(way).wait_send()
    out = blocks.at[pl.ds(0, (last * PIECES + half) * size - EARLY)]
    for way, to in enumerate((after, before)):
        pltpu.make_async_remote_copy(
            out, out, sent_sem.at[way], right_recv.at[0], device_id={"zero": to}, device_id_type=MESH
        ).wait_send()
    whole_line().wait_send()
    for k in range(turns):
        plane_copy(k).wait_send()


def place_kernel(n, rows, thin, blocks, *refs):
    query, key, value = refs[4:7]
    sems = refs[-1]
    wide = rows + 2 * thin
    for z in range(n):
        here = pl.ds(z * rows, rows)
        pltpu.make_async_copy(blocks.at[pl.ds(z * wide, rows)], query.at[here], sems.at[0]).start()
        pltpu.make_async_copy(blocks.at[pl.ds(z * wide + rows, thin)], key.at[:, here], sems.at[1]).start()
        pltpu.make_async_copy(blocks.at[pl.ds(z * wide + rows + thin, thin)], value.at[:, here], sems.at[2]).start()
    small = [
        pltpu.make_async_copy(src, dst, sems.at[3 + k]) for k, (src, dst) in enumerate(zip(refs[:4], refs[7:11]))
    ]
    for copy in small:
        copy.start()
    for copy in small:
        copy.wait()
    for k, large in enumerate((query, key, value)):
        pltpu.make_async_copy(large, large, sems.at[k]).wait()


def on_device(first_q, second_q, first_k, second_k, first_v, second_v, mix, train, step):
    n, m = lax.axis_size("zero"), lax.axis_size("model")
    rows, cols = first_q.shape
    thin = first_k.shape[1]
    wide = rows + 2 * thin
    piece = train.shape[0]
    tiles = rows // LANES
    f32, bf16 = jnp.float32, jnp.bfloat16
    anywhere = pl.BlockSpec(memory_space=pltpu.HBM)
    vmem = pl.BlockSpec(memory_space=pltpu.VMEM)
    dma = pltpu.SemaphoreType.DMA
    norm_rows = n * m * piece // LANES
    hbm = lambda x: pltpu.with_memory_space_constraint(x, pltpu.HBM)
    blocks, *small = pl.pallas_call(
        gather_kernel,
        out_shape=(
            pltpu.VMEM((n * wide, cols), bf16),
            pltpu.VMEM((tiles, LANES), f32),
            pltpu.VMEM((1, thin), f32),
            pltpu.VMEM((1, thin), f32),
            pltpu.VMEM((norm_rows, LANES), bf16),
        ),
        in_specs=[anywhere] * 9,
        out_specs=(vmem,) * 5,
        scratch_shapes=[
            pltpu.VMEM((rows, cols), f32),
            pltpu.VMEM((rows, cols), f32),
            pltpu.VMEM((2 * thin, rows), f32),
            pltpu.VMEM((2 * thin, rows), f32),
            pltpu.VMEM((1, rows), f32),
            pltpu.VMEM((rows, LANES), f32),
            pltpu.VMEM((2, 1, piece), f32),
            pltpu.VMEM((8, LANES), f32),
            pltpu.VMEM((wide, cols), f32),
            pltpu.VMEM((n, tiles + 2, 1, LANES), f32),
            pltpu.VMEM((m, n, LANES), f32),
            pltpu.VMEM((norm_rows, LANES), f32),
            pltpu.VMEM((2, max(EARLY, 8), cols), f32),
            dma((7 + 2 * tiles,)),
            dma((2,)),
            dma((2 * (math.isqrt(m) - 1),)),
            dma((2 * (math.isqrt(m) - 1),)),
            dma((2,)),
            dma((2,)),
            dma((2,)),
            dma((n // 2 * PIECES,)),
            dma((n // 2 * PIECES,)),
        ],
        compiler_params=pltpu.CompilerParams(
            collective_id=0, has_side_effects=True, vmem_limit_bytes=24 * 1024 * 1024
        ),
        name="gather",
    )(
        hbm(first_q), hbm(second_q), hbm(first_k.T), hbm(second_k.T), hbm(first_v.T), hbm(second_v.T),
        hbm(mix.reshape(1, rows)), hbm(train.reshape(1, piece)), hbm(step.reshape(1, piece)),
    )
    query, key, value, f_query, f_key, f_value, norm = pl.pallas_call(
        functools.partial(place_kernel, n, rows, thin),
        out_shape=(
            jax.ShapeDtypeStruct((n * rows, cols), bf16),
            jax.ShapeDtypeStruct((thin, n * rows), bf16),
            jax.ShapeDtypeStruct((thin, n * rows), bf16),
            jax.ShapeDtypeStruct((tiles, LANES), f32),
            jax.ShapeDtypeStruct((1, thin), f32),
            jax.ShapeDtypeStruct((1, thin), f32),
            jax.ShapeDtypeStruct((norm_rows, LANES), bf16),
        ),
        in_specs=[vmem] * 5,
        out_specs=(anywhere,) * 7,
        scratch_shapes=[dma((7,))],
        compiler_params=pltpu.CompilerParams(vmem_limit_bytes=24 * 1024 * 1024),
        name="place",
    )(blocks, *small)
    return (
        query, key.T, value.T,
        f_query.reshape(-1), f_key.reshape(-1), f_value.reshape(-1), norm.reshape(-1),
    )


def solution(mesh):
    own = P(("unit", "zero"), "model")
    return jax.shard_map(
        on_device,
        mesh=mesh,
        in_specs=(own, own, own, own, own, own, P(("unit", "zero")), P(("unit", "zero", "model")), P(("unit", "zero", "model"))),
        out_specs=(
            P("unit", "model"), P("unit", "model"), P("unit", "model"),
            P(("unit", "model")), P(("unit", "model")), P(("unit", "model")), P("unit"),
        ),
        check_vma=False,
    )
```

```python
import functools
import math

import jax
import jax.numpy as jnp
from jax import lax
from jax.experimental import pallas as pl
from jax.experimental.pallas import tpu as pltpu
from jax.sharding import PartitionSpec as P

MESH = pl.DeviceIdType.MESH
LANES = 128
PIECES = 4
EARLY = 96


def gather_kernel(
    first_q, second_q, first_k, second_k, first_v, second_v, mix, train, step,
    blocks, f_query, f_key, f_value, norm,
    a_q, b_q, a_kv, b_kv, mix_row, share, norm_in, lane_row, fresh, stat, plane, norm_wide, early,
    load_sem, line_sem, plane_send, plane_recv, early_send, early_recv, sent_sem, right_recv, left_recv,
):
    n, m = lax.axis_size("zero"), lax.axis_size("model")
    me, col = lax.axis_index("zero"), lax.axis_index("model")
    rows, cols = first_q.shape
    thin = first_k.shape[0]
    wide = rows + 2 * thin
    size = wide // PIECES
    half = PIECES // 2
    tiles = rows // LANES
    side = math.isqrt(m)
    across, down = lax.rem(col, side), col // side

    def beside(d):
        return down * side + lax.rem(across + d, side)

    def below(d):
        return lax.rem(down + d, side) * side + across

    def load(k, src, dst):
        return pltpu.make_async_copy(src, dst, load_sem.at[k])

    load_mix = load(0, mix, mix_row)
    load_thin = [
        load(1, first_k, a_kv.at[pl.ds(0, thin)]),
        load(2, second_k, b_kv.at[pl.ds(0, thin)]),
        load(3, first_v, a_kv.at[pl.ds(thin, thin)]),
        load(4, second_v, b_kv.at[pl.ds(thin, thin)]),
    ]
    load_gain = [load(5, train, norm_in.at[0]), load(6, step, norm_in.at[1])]
    load_q = []
    for r in range(tiles):
        part = pl.ds(r * LANES, LANES)
        load_q.append(
            (load(7 + 2 * r, first_q.at[part], a_q.at[part]), load(8 + 2 * r, second_q.at[part], b_q.at[part]))
        )

    def around(d):
        return {"zero": lax.rem(me + d, n)}

    barrier = pltpu.get_barrier_semaphore()

    outward = [n // 2]
    for d in range(n // 2 - 1, 0, -1):
        outward += [d, n - d]
    for d in outward:
        pl.semaphore_signal(barrier, inc=1, device_id=around(d), device_id_type=MESH)
    for peer in (beside(side - 1), below(side - 1)):
        pl.semaphore_signal(barrier, inc=1, device_id={"model": peer}, device_id_type=MESH)
    load_mix.start()
    for copy in load_thin:
        copy.start()
    for pair in load_q:
        for copy in pair:
            copy.start()
    for copy in load_gain:
        copy.start()

    load_mix.wait()
    for r in range(tiles):
        row = mix_row[:, r * LANES : (r + 1) * LANES]
        share[r * LANES : (r + 1) * LANES, :] = jnp.broadcast_to(row, (LANES, LANES)).T

    sums = [jnp.zeros((8, LANES), jnp.float32) for _ in range(tiles)]
    for r in range(tiles):
        if r == tiles - 1:
            for copy in load_thin:
                copy.wait()
            w = mix_row[...]
            f = w * a_kv[...] + (1.0 - w) * b_kv[...]
            fresh[rows:, :] = f
            s = f * f
            folded = s[:, :LANES]
            for c in range(1, tiles):
                folded = folded + s[:, c * LANES : (c + 1) * LANES]
            stat[me, tiles] = jnp.sum(folded.T, axis=0, keepdims=True)
        for copy in load_q[r]:
            copy.wait()
        part = slice(r * LANES, (r + 1) * LANES)
        w = share[part, :]
        for c in range(tiles):
            lanes = slice(c * LANES, (c + 1) * LANES)
            f = w * a_q[part, lanes] + (1.0 - w) * b_q[part, lanes]
            fresh[part, lanes] = f
            sums[c] = sums[c] + jnp.sum((f * f).reshape(LANES // 8, 8, LANES), axis=0)
    for c in range(tiles):
        stat[me, c] = jnp.sum(sums[c], axis=0, keepdims=True)

    for copy in load_gain:
        copy.wait()
    gain = (norm_in[0] + norm_in[1]).astype(jnp.bfloat16).astype(jnp.float32)
    lane_row[...] = jnp.zeros_like(lane_row)
    share_of_row = gain.shape[1]
    per_row = LANES // share_of_row
    lane_row[0:1, 0:share_of_row] = gain
    gain = lane_row[...]
    spread = gain
    for k in range(1, per_row):
        spread = spread + pltpu.roll(gain, k * share_of_row, 1)
    lane = lax.broadcasted_iota(jnp.int32, (8, LANES), 1)
    spread = jnp.where(lane // share_of_row == lax.rem(col, per_row), spread, 0.0)

    stat[me, tiles + 1] = spread[0:1, :]

    pl.semaphore_wait(barrier, n - 1 + 2)

    def to_line(d):
        return pltpu.make_async_remote_copy(
            stat.at[me], stat.at[me], line_sem.at[0], line_sem.at[1], device_id=around(d), device_id_type=MESH
        )

    def whole_line():
        every = stat.at[pl.ds(0, n - 1)]
        return pltpu.make_async_remote_copy(
            every, every, line_sem.at[0], line_sem.at[1], device_id=around(1), device_id_type=MESH
        )

    for d in outward:
        to_line(d).start()

    after, before = lax.rem(me + 1, n), lax.rem(me + n - 1, n)

    def early_copy(way):
        return pltpu.make_async_remote_copy(
            fresh.at[pl.ds(0, EARLY)], early.at[way], early_send.at[way], early_recv.at[way],
            device_id={"zero": (after, before)[way]}, device_id_type=MESH,
        )

    ways = (0, 1) if EARLY else ()
    for way in ways:
        early_copy(way).start()

    whole_line().wait_recv()

    def factor_of(c):
        total = stat[0, c]
        for z in range(1, n):
            total = total + stat[z, c]
        return jnp.sqrt(total)

    factor = [factor_of(c) for c in range(tiles)]
    inverse = [1.0 / f for f in factor]

    def rounded(source, owner, low, high):
        base = pl.multiple_of(owner * wide, wide)
        edge = min(max(rows, low), high)
        if low < edge:
            for c in range(tiles):
                lanes = slice(c * LANES, (c + 1) * LANES)
                blocks[pl.ds(base + low, edge - low), lanes] = (source[low:edge, lanes] * inverse[c]).astype(jnp.bfloat16)
        if edge < high:
            scale = thin_inverse[0][edge - rows : high - rows, :]
            for c in range(tiles):
                lanes = slice(c * LANES, (c + 1) * LANES)
                blocks[pl.ds(base + edge, high - edge), lanes] = (source[edge:high, lanes] * scale).astype(jnp.bfloat16)

    def piece_copy(way, recv, origin, s, p, to):
        skip = EARLY if s == 0 and p == 0 else 0
        start = pl.multiple_of(origin * wide + p * size + skip, 16)
        where = blocks.at[pl.ds(start, size - skip)]
        return pltpu.make_async_remote_copy(
            where, where, sent_sem.at[way], recv.at[s * PIECES + p],
            device_id={"zero": to}, device_id_type=MESH,
        )

    def to_right(s, p):
        return piece_copy(0, right_recv, lax.rem(me + n - s, n), s, p, after)

    def to_left(s, p):
        return piece_copy(1, left_recv, lax.rem(me + s, n), s, p, before)

    def from_left(s, p):
        return piece_copy(0, right_recv, lax.rem(before + n - s, n), s, p, after)

    def from_right(s, p):
        return piece_copy(1, left_recv, lax.rem(after + s, n), s, p, before)

    thin_inverse = []
    for p in range(PIECES):
        rounded(fresh, me, p * size if p else EARLY, (p + 1) * size)
        if p == 0:
            thin_factor = factor_of(tiles)
            thin_inverse.append(jnp.broadcast_to(1.0 / thin_factor, (LANES, LANES)).T)
            for c in range(tiles):
                f_query[c : c + 1, :] = factor[c]
            f_key[...] = thin_factor[:, :thin]
            f_value[...] = thin_factor[:, thin:]
            to_right(0, 0).start()
            to_left(0, 0).start()
        if p > 1:
            to_right(0, p - 1).start()
            to_left(0, p - 1).start()
    if EARLY:
        rounded(fresh, me, 0, EARLY)
    to_right(0, PIECES - 1).start()
    to_left(0, PIECES - 1).start()
    for way in ways:
        early_copy(way).wait_recv()
        rounded(early.at[way], (before, after)[way], 0, EARLY)

    for z in range(n):
        plane[col, z : z + 1, :] = stat[z, tiles + 1]

    def plane_copy(k):
        if k < side - 1:
            slot = plane.at[pl.ds(beside(side - k), 1)]
            to = beside(1)
        else:
            slot = plane.at[pl.ds(lax.rem(down + side - (k - side + 1), side) * side, side)]
            to = below(1)
        return pltpu.make_async_remote_copy(
            slot, slot, plane_send.at[k], plane_recv.at[k], device_id={"model": to}, device_id_type=MESH
        )

    def plane_from(k):
        if k < side - 1:
            slot = plane.at[pl.ds(beside(2 * side - 1 - k), 1)]
            to = beside(1)
        else:
            slot = plane.at[pl.ds(lax.rem(down + 2 * side - 1 - (k - side + 1), side) * side, side)]
            to = below(1)
        return pltpu.make_async_remote_copy(
            slot, slot, plane_send.at[k], plane_recv.at[k], device_id={"model": to}, device_id_type=MESH
        )

    last = n // 2 - 1
    turns = 2 * (side - 1)
    plane_copy(0).start()
    for s in range(1, last):

        def one(p, c):
            from_left(s - 1, p).wait_recv()
            to_right(s, p).start()
            from_right(s - 1, p).wait_recv()
            to_left(s, p).start()
            return c

        for p in range(PIECES):
            one(p, 0)
        if s <= turns:
            plane_from(s - 1).wait_recv()
            if s < turns:
                plane_copy(s).start()
    for k in range(max(last - 1, 0), turns):
        plane_from(k).wait_recv()
        if k + 1 < turns:
            plane_copy(k + 1).start()

    per = m // per_row
    for k in range(per):
        line = plane[k * per_row]
        for j in range(1, per_row):
            line = line + plane[k * per_row + j]
        norm_wide[pl.ds(k, n, stride=per), :] = line
    norm[...] = norm_wide[...].astype(jnp.bfloat16)

    def near(p, c):
        from_left(last - 1, p).wait_recv()
        to_right(last, p).start()
        from_right(last - 1, p + half).wait_recv()
        to_left(last, p + half).start()
        return c

    def far(p, c):
        from_right(last - 1, p).wait_recv()
        from_left(last - 1, p + half).wait_recv()
        return c

    def end(p, c):
        from_left(last, p).wait_recv()
        from_right(last, p + half).wait_recv()
        return c

    lax.fori_loop(0, half, near, 0)
    lax.fori_loop(0, half, far, 0)
    lax.fori_loop(0, half, end, 0)

    for way in ways:
        early_copy(way).wait_send()
    out = blocks.at[pl.ds(0, (last * PIECES + half) * size - EARLY)]
    for way, to in enumerate((after, before)):
        pltpu.make_async_remote_copy(
            out, out, sent_sem.at[way], right_recv.at[0], device_id={"zero": to}, device_id_type=MESH
        ).wait_send()
    whole_line().wait_send()
    for k in range(turns):
        plane_copy(k).wait_send()


def place_kernel(n, rows, thin, blocks, *refs):
    query, key, value = refs[4:7]
    sems = refs[-1]
    wide = rows + 2 * thin
    for z in range(n):
        here = pl.ds(z * rows, rows)
        pltpu.make_async_copy(blocks.at[pl.ds(z * wide, rows)], query.at[here], sems.at[0]).start()
        pltpu.make_async_copy(blocks.at[pl.ds(z * wide + rows, thin)], key.at[:, here], sems.at[1]).start()
        pltpu.make_async_copy(blocks.at[pl.ds(z * wide + rows + thin, thin)], value.at[:, here], sems.at[2]).start()
    small = [
        pltpu.make_async_copy(src, dst, sems.at[3 + k]) for k, (src, dst) in enumerate(zip(refs[:4], refs[7:11]))
    ]
    for copy in small:
        copy.start()
    for copy in small:
        copy.wait()
    for k, large in enumerate((query, key, value)):
        pltpu.make_async_copy(large, large, sems.at[k]).wait()


def on_device(first_q, second_q, first_k, second_k, first_v, second_v, mix, train, step):
    n, m = lax.axis_size("zero"), lax.axis_size("model")
    rows, cols = first_q.shape
    thin = first_k.shape[1]
    wide = rows + 2 * thin
    piece = train.shape[0]
    tiles = rows // LANES
    f32, bf16 = jnp.float32, jnp.bfloat16
    anywhere = pl.BlockSpec(memory_space=pltpu.HBM)
    vmem = pl.BlockSpec(memory_space=pltpu.VMEM)
    dma = pltpu.SemaphoreType.DMA
    norm_rows = n * m * piece // LANES
    hbm = lambda x: pltpu.with_memory_space_constraint(x, pltpu.HBM)
    blocks, *small = pl.pallas_call(
        gather_kernel,
        out_shape=(
            pltpu.VMEM((n * wide, cols), bf16),
            pltpu.VMEM((tiles, LANES), f32),
            pltpu.VMEM((1, thin), f32),
            pltpu.VMEM((1, thin), f32),
            pltpu.VMEM((norm_rows, LANES), bf16),
        ),
        in_specs=[anywhere] * 9,
        out_specs=(vmem,) * 5,
        scratch_shapes=[
            pltpu.VMEM((rows, cols), f32),
            pltpu.VMEM((rows, cols), f32),
            pltpu.VMEM((2 * thin, rows), f32),
            pltpu.VMEM((2 * thin, rows), f32),
            pltpu.VMEM((1, rows), f32),
            pltpu.VMEM((rows, LANES), f32),
            pltpu.VMEM((2, 1, piece), f32),
            pltpu.VMEM((8, LANES), f32),
            pltpu.VMEM((wide, cols), f32),
            pltpu.VMEM((n, tiles + 2, 1, LANES), f32),
            pltpu.VMEM((m, n, LANES), f32),
            pltpu.VMEM((norm_rows, LANES), f32),
            pltpu.VMEM((2, max(EARLY, 8), cols), f32),
            dma((7 + 2 * tiles,)),
            dma((2,)),
            dma((2 * (math.isqrt(m) - 1),)),
            dma((2 * (math.isqrt(m) - 1),)),
            dma((2,)),
            dma((2,)),
            dma((2,)),
            dma((n // 2 * PIECES,)),
            dma((n // 2 * PIECES,)),
        ],
        compiler_params=pltpu.CompilerParams(
            collective_id=0, has_side_effects=True, vmem_limit_bytes=24 * 1024 * 1024
        ),
        name="gather",
    )(
        hbm(first_q), hbm(second_q), hbm(first_k.T), hbm(second_k.T), hbm(first_v.T), hbm(second_v.T),
        hbm(mix.reshape(1, rows)), hbm(train.reshape(1, piece)), hbm(step.reshape(1, piece)),
    )
    query, key, value, f_query, f_key, f_value, norm = pl.pallas_call(
        functools.partial(place_kernel, n, rows, thin),
        out_shape=(
            jax.ShapeDtypeStruct((n * rows, cols), bf16),
            jax.ShapeDtypeStruct((thin, n * rows), bf16),
            jax.ShapeDtypeStruct((thin, n * rows), bf16),
            jax.ShapeDtypeStruct((tiles, LANES), f32),
            jax.ShapeDtypeStruct((1, thin), f32),
            jax.ShapeDtypeStruct((1, thin), f32),
            jax.ShapeDtypeStruct((norm_rows, LANES), bf16),
        ),
        in_specs=[vmem] * 5,
        out_specs=(anywhere,) * 7,
        scratch_shapes=[dma((7,))],
        compiler_params=pltpu.CompilerParams(vmem_limit_bytes=24 * 1024 * 1024),
        name="place",
    )(blocks, *small)
    return (
        query, key.T, value.T,
        f_query.reshape(-1), f_key.reshape(-1), f_value.reshape(-1), norm.reshape(-1),
    )


def solution(mesh):
    own = P(("unit", "zero"), "model")
    return jax.shard_map(
        on_device,
        mesh=mesh,
        in_specs=(own, own, own, own, own, own, P(("unit", "zero")), P(("unit", "zero", "model")), P(("unit", "zero", "model"))),
        out_specs=(
            P("unit", "model"), P("unit", "model"), P("unit", "model"),
            P(("unit", "model")), P(("unit", "model")), P(("unit", "model")), P("unit"),
        ),
        check_vma=False,
    )
```
